256 devices in a mesh: col: 32 (over z, y), row: 8 (over x, core).
Axes of the slice: x: 4, y: 4, z: 8, core: 2. Of those that a mesh axis runs over, the one named last changes fastest.
Arguments:
- w_gate: float32 [2048, 5120], P('row', 'col')
- w_up: float32 [2048, 5120], P('row', 'col')
- w_down: float32 [5120, 2048], P('row', 'col')
- x_norm: bfloat16 [16384, 2048], P(None, 'row')
- x_act: bfloat16 [16384, 5120], P(None, 'row')
- dy_gate: bfloat16 [16384, 5120], P(None, 'col')
- dy_up: bfloat16 [16384, 5120], P(None, 'col')
- dy_down: bfloat16 [16384, 2048], P(None, 'col')
- r_gate: float32 [2048], P('row')
- c_gate: float32 [5120], P('col')
- r_up: float32 [2048], P('row')
- c_up: float32 [5120], P('col')
- r_down: float32 [5120], P('row')
- c_down: float32 [2048], P('col')
- hyper_params: float32 [3], replicated
Outputs:
- output 1: float32 [2048, 5120], P('row', 'col')
- output 2: float32 [2048, 5120], P('row', 'col')
- output 3: float32 [5120, 2048], P('row', 'col')
- output 4: float32 [2048], P('row')
- output 5: float32 [5120], P('col')
- output 6: float32 [2048], P('row')
- output 7: float32 [5120], P('col')
- output 8: float32 [5120], P('row')
- output 9: float32 [2048], P('col')
- output 10: bfloat16 [16384, 2048], P(None, 'row')
- output 11: bfloat16 [16384, 5120], P(None, 'row')
All inputs are finite; a program needn't handle non-finite values.
Results may differ from the reference program's by a relative error of at most 0.001.
Values are sent between devices in bfloat16 or wider.
A program may use at most 768 MiB of HBM per device.

```python
import jax
import jax.numpy as jnp
from jax import lax

D_MODEL = 2048
D_FF = 5120
TOKENS = 16384
EPS_ONE = 1e-30
EPS_TWO = 1e-3
TWO_PI = 6.283185307179586


def smooth_field(key, length, log_scale):
    key_amp, key_phase = jax.random.split(key)
    ampl_k = jax.random.normal(key_amp, (3,), jnp.float32)
    phase_k = jax.random.uniform(key_phase, (3,), jnp.float32, minval=0.0, maxval=TWO_PI)
    position = jnp.arange(length, dtype=jnp.float32) / length
    freq_k = jnp.arange(1, 4, dtype=jnp.float32)
    waves = jnp.cos(TWO_PI * position[:, None] * freq_k[None, :] + phase_k[None, :])
    return jnp.exp(log_scale * jnp.sum(waves * ampl_k[None, :], axis=1) / 1.7)


def draw_weight(key, rows, cols):
    key_z, key_r, key_c = jax.random.split(key, 3)
    noise = jax.random.normal(key_z, (rows, cols), jnp.float32)
    row_prof = smooth_field(key_r, rows, 0.5)
    col_prof = smooth_field(key_c, cols, 0.5)
    return noise * (rows ** -0.5) * row_prof[:, None] * col_prof[None, :]


def draw_tokens(key, cols, scale):
    key_z, key_a, key_b = jax.random.split(key, 3)
    noise = jax.random.normal(key_z, (TOKENS, cols), jnp.float32)
    first_half = (jnp.arange(TOKENS) < TOKENS // 2)[:, None]
    profile = jnp.where(first_half, smooth_field(key_a, cols, 0.8)[None, :], smooth_field(key_b, cols, 0.8)[None, :])
    return (noise * profile * scale).astype(jnp.bfloat16)


def draw_stat(key, length):
    return jax.random.uniform(key, (length,), jnp.float32, minval=0.5, maxval=3.0)


def setup_inputs(seed: int = 0) -> dict:
    keys = jax.random.split(jax.random.key(seed), 15)
    tok_scale = TOKENS ** -0.5
    low_end = jnp.array([0.6, 0.6, 0.15], dtype=jnp.float32)
    span_len = jnp.array([0.25, 0.6, 0.15], dtype=jnp.float32)
    unit_draw = jax.random.uniform(keys[14], (3,), jnp.float32)
    return {
        'w_gate': draw_weight(keys[0], D_MODEL, D_FF),
        'w_up': draw_weight(keys[1], D_MODEL, D_FF),
        'w_down': draw_weight(keys[2], D_FF, D_MODEL),
        'x_norm': draw_tokens(keys[3], D_MODEL, tok_scale),
        'x_act': draw_tokens(keys[4], D_FF, tok_scale),
        'dy_gate': draw_tokens(keys[5], D_FF, 1.0),
        'dy_up': draw_tokens(keys[6], D_FF, 1.0),
        'dy_down': draw_tokens(keys[7], D_MODEL, 1.0),
        'r_gate': draw_stat(keys[8], D_MODEL),
        'c_gate': draw_stat(keys[9], D_FF),
        'r_up': draw_stat(keys[10], D_MODEL),
        'c_up': draw_stat(keys[11], D_FF),
        'r_down': draw_stat(keys[12], D_FF),
        'c_down': draw_stat(keys[13], D_MODEL),
        'hyper_params': low_end + span_len * unit_draw,
    }


def factored_step(w_old, grad_w, r_old, c_old, hyper_params):
    beta_two = hyper_params[0]
    grad_sq = grad_w * grad_w + EPS_ONE
    r_new = beta_two * r_old + (1.0 - beta_two) * jnp.mean(grad_sq, axis=1)
    c_new = beta_two * c_old + (1.0 - beta_two) * jnp.mean(grad_sq, axis=0)
    v_est = r_new[:, None] * c_new[None, :] / jnp.mean(r_new)
    update = grad_w * lax.rsqrt(v_est)
    rms_u = jnp.sqrt(jnp.mean(update * update))
    update_hat = update / jnp.maximum(1.0, rms_u / hyper_params[2])
    step_size = hyper_params[1] * jnp.maximum(EPS_TWO, jnp.sqrt(jnp.mean(w_old * w_old)))
    return w_old - step_size * update_hat, r_new, c_new


def weight_grad(activations, grad_out):
    return jnp.dot(activations.T, grad_out, preferred_element_type=jnp.float32)


def input_grad(grad_out, weight):
    return jnp.dot(grad_out, weight.astype(jnp.bfloat16).T, preferred_element_type=jnp.float32)


def reference(w_gate, w_up, w_down, x_norm, x_act, dy_gate, dy_up, dy_down, r_gate, c_gate, r_up, c_up, r_down, c_down, hyper_params):
    new_gate, r_gate_new, c_gate_new = factored_step(w_gate, weight_grad(x_norm, dy_gate), r_gate, c_gate, hyper_params)
    new_up, r_up_new, c_up_new = factored_step(w_up, weight_grad(x_norm, dy_up), r_up, c_up, hyper_params)
    new_down, r_down_new, c_down_new = factored_step(w_down, weight_grad(x_act, dy_down), r_down, c_down, hyper_params)
    dx_norm = (input_grad(dy_gate, w_gate) + input_grad(dy_up, w_up)).astype(jnp.bfloat16)
    dx_act = input_grad(dy_down, w_down).astype(jnp.bfloat16)
    return (new_gate, new_up, new_down, r_gate_new, c_gate_new, r_up_new, c_up_new, r_down_new, c_down_new, dx_norm, dx_act)
```

```python
import jax
import jax.numpy as jnp
from jax import lax
from jax.experimental import pallas as pl
from jax.experimental.pallas import tpu as pltpu
from jax.sharding import PartitionSpec as P

EPS_ONE = 1e-30
EPS_TWO = 1e-3
MESH = pl.DeviceIdType.MESH
NY, NZ, NX = 4, 8, 4
NCOL, NROW = NY * NZ, NX * 2
LONG = NCOL // 2
BF16, F32 = jnp.bfloat16, jnp.float32


def ring_place(cycle, col):
    y, z = col % NY, col // NY
    u = (y + z) % NY
    if cycle == 0:
        return NY * z + u
    return NY * ((3 * (z - u + NZ)) % NZ) + u


def ring_col(cycle, place):
    place = (place + NCOL) % NCOL
    q, u = place // NY, place % NY
    z = q if cycle == 0 else (3 * q + u) % NZ
    return z * NY + (u - z + NZ) % NY


class Rings:
    def __init__(self, col, row, parts, send_sems, recv_sems):
        self.row, self.parts, self.send_sems, self.recv_sems = row, parts, send_sems, recv_sems
        sign = 1 - 2 * (row % 2)
        self.lanes = []
        for cycle in range(2):
            place = ring_place(cycle, col)
            for way in range(2):
                step_dir = sign if way == 0 else -sign
                self.lanes.append((cycle, way, place, step_dir, ring_col(cycle, place + step_dir)))

    def copies(self, lane, step):
        cycle, way, place, step_dir, peer = self.lanes[lane]
        origin = ring_col(cycle, place - step_dir * step)
        return [
            pltpu.make_async_remote_copy(
                src_ref=part(cycle, origin), dst_ref=part(cycle, origin),
                send_sem=self.send_sems.at[lane, step, k], recv_sem=self.recv_sems.at[lane, step, k],
                device_id=(peer, self.row), device_id_type=MESH)
            for k, part in enumerate(self.parts)
        ]

    def n_steps(self, lane):
        return LONG - self.lanes[lane][1]

    def start(self, step):
        for lane in range(4):
            def go(lane=lane):
                for copy in self.copies(lane, step):
                    copy.start()
            if isinstance(step, int):
                go()
            else:
                pl.when(step < self.n_steps(lane))(go)

    def wait_recv(self, step):
        for lane in range(4):
            def go(lane=lane):
                for copy in self.copies(lane, step):
                    copy.wait_recv()
            if isinstance(step, int):
                if step < self.n_steps(lane):
                    go()
            else:
                pl.when(step < self.n_steps(lane))(go)

    def wait_sends(self):
        for lane in range(4):
            @pl.loop(0, self.n_steps(lane))
            def _(step, lane=lane):
                for copy in self.copies(lane, step):
                    copy.wait_send()


def exchange_kernel(dy_ref, wn_ref, wa_ref, dxn_ref, dxa_ref, dy_all, wn_all, wa_all, acc_n, acc_a,
                    ring_send, ring_recv, local_sem, a2a_sems, x_send, x_recv):
    col, row = lax.axis_index('col'), lax.axis_index('row')
    x, core = row // 2, row % 2
    slice_len = dy_ref.shape[0] // NCOL
    sub = slice_len // NROW
    nn, na = wn_ref.shape[0], wa_ref.shape[0]
    width = dy_ref.shape[1]
    pad_n, pad_a = width - nn, wa_all.shape[1] - na

    own_w = [pltpu.make_async_copy(wn_ref, wn_all.at[col, pl.ds(0, nn)], local_sem.at[0]),
             pltpu.make_async_copy(wa_ref, wa_all.at[col, pl.ds(pad_a, na)], local_sem.at[1])]
    for copy in own_w:
        copy.start()

    def a2a(peer):
        tokens = pl.ds(pl.multiple_of(peer * slice_len + row * sub, sub), sub)
        return dy_ref.at[tokens], dy_all.at[row, col]

    for copy in own_w:
        copy.wait()
    rings = Rings(col, row, [
        lambda cycle, origin: wn_all.at[origin, pl.ds(cycle * (nn // 2), nn // 2)],
        lambda cycle, origin: wa_all.at[origin, pl.ds(pad_a + cycle * (na // 2), na // 2)]], ring_send, ring_recv)
    rings.start(0)

    src, dst = a2a(col)
    pltpu.make_async_copy(src, dst, a2a_sems.at[1]).start()

    @pl.loop(1, NCOL)
    def _(shift):
        peer = (col + shift) % NCOL
        src, dst = a2a(peer)
        pltpu.make_async_remote_copy(src_ref=src, dst_ref=dst, send_sem=a2a_sems.at[0], recv_sem=a2a_sems.at[1],
                                     device_id=(peer, row), device_id_type=MESH).start()

    wn_all[:, pl.ds(nn, pad_n), :] = jnp.zeros((NCOL, pad_n, wn_all.shape[2]), BF16)
    wa_all[:, pl.ds(0, pad_a), :] = jnp.zeros((NCOL, pad_a, wa_all.shape[2]), BF16)

    def row_of(dx):
        return ((x + dx + NX) % NX) * 2 + core

    partner = x * 2 + 1 - core
    half = NCOL // 2

    def hop(k, slot, target, cols=None):
        ref = dy_all.at[slot] if cols is None else dy_all.at[slot, cols]
        return pltpu.make_async_remote_copy(src_ref=ref, dst_ref=ref, send_sem=x_send.at[k], recv_sem=x_recv.at[k],
                                            device_id=(col, target), device_id_type=MESH)

    own, prev, succ, far = row, row_of(-1), row_of(1), row_of(2)
    low, high = pl.ds(0, half), pl.ds(half, half)
    hops = [
        hop(0, own, succ), hop(1, own, prev), hop(2, own, partner),
        hop(3, prev, succ, low), hop(4, prev, partner),
        hop(5, succ, prev, high), hop(6, succ, partner),
        hop(7, far, partner, low), hop(8, far, partner, high)]

    def ring_steps(first, last):
        @pl.loop(first, last)
        def _(step):
            rings.wait_recv(step - 1)
            rings.start(step)

    ring_steps(1, 4)
    pltpu.make_async_copy(dy_all.at[row], dy_all.at[row], a2a_sems.at[1]).wait()
    for k in (0, 1, 2):
        hops[k].start()
    ring_steps(4, 11)
    hops[0].wait_recv()
    hops[3].start()
    hops[4].start()
    hops[1].wait_recv()
    hops[5].start()
    hops[6].start()
    ring_steps(11, LONG)
    hops[3].wait_recv()
    hops[7].start()
    hops[5].wait_recv()
    hops[8].start()
    rings.wait_recv(LONG - 1)
    for k in (2, 4, 6, 7, 8):
        hops[k].wait_recv()

    tokens = NROW * sub
    lo = (nn // 128) * 128

    @pl.loop(0, NCOL // 2)
    def _(pair):
        j = pair * 2
        d0 = dy_all[:, j, :, :].reshape(tokens, width)
        d1 = dy_all[:, j + 1, :, :].reshape(tokens, width)
        part_n = (jnp.dot(jnp.concatenate([d0, d1], axis=1), wn_all[pl.ds(j, 2)].reshape(2 * width, wn_all.shape[2]),
                          preferred_element_type=F32))
        part_a = jnp.dot(jnp.concatenate([d0[:, lo:], d1[:, lo:]], axis=1),
                         wa_all[pl.ds(j, 2)].reshape(2 * wa_all.shape[1], wa_all.shape[2]), preferred_element_type=F32)

        @pl.when(pair == 0)
        def _():
            acc_n[...] = part_n
            acc_a[...] = part_a

        @pl.when(pair > 0)
        def _():
            acc_n[...] += part_n
            acc_a[...] += part_a

    dxn_ref[...] = acc_n[...].astype(BF16)
    dxa_ref[...] = acc_a[...].astype(BF16)

    for k in range(9):
        hops[k].wait_send()
    sent = dy_all.at[row, pl.ds(0, NCOL - 1)]
    pltpu.make_async_copy(sent, sent, a2a_sems.at[0]).wait()
    rings.wait_sends()


def exchange(dy, wn, wa):
    tokens = dy.shape[0] // NCOL
    width = dy.shape[1]
    vmem = pl.BlockSpec(memory_space=pltpu.VMEM)
    pad_rows = width - (wn.shape[0] // 128) * 128
    return pl.pallas_call(
        exchange_kernel,
        out_shape=(jax.ShapeDtypeStruct((tokens, wn.shape[1]), BF16), jax.ShapeDtypeStruct((tokens, wa.shape[1]), BF16)),
        in_specs=[pl.BlockSpec(memory_space=pl.ANY), vmem, vmem],
        out_specs=(vmem, vmem),
        scratch_shapes=[
            pltpu.VMEM((NROW, NCOL, tokens // NROW, width), BF16),
            pltpu.VMEM((NCOL, width, wn.shape[1]), BF16),
            pltpu.VMEM((NCOL, pad_rows, wa.shape[1]), BF16),
            pltpu.VMEM((tokens, wn.shape[1]), F32),
            pltpu.VMEM((tokens, wa.shape[1]), F32),
            pltpu.SemaphoreType.DMA((4, LONG, 2)),
            pltpu.SemaphoreType.DMA((4, LONG, 2)),
            pltpu.SemaphoreType.DMA((2,)),
            pltpu.SemaphoreType.DMA((2,)),
            pltpu.SemaphoreType.DMA((9,)),
            pltpu.SemaphoreType.DMA((9,)),
        ],
        compiler_params=pltpu.CompilerParams(has_side_effects=True, vmem_limit_bytes=60 * 1024 * 1024),
        name='exchange',
    )(dy, wn, wa)


def factored_step(w_loc, grad_loc, r_loc, c_loc, hyper_params, m_total, n_total):
    beta_two = hyper_params[0]
    grad_sq = grad_loc * grad_loc + EPS_ONE
    row_sum = lax.psum(jnp.sum(grad_sq, axis=1), 'col')
    col_sum = lax.psum(jnp.sum(grad_sq, axis=0), 'row')
    r_new = beta_two * r_loc + (1.0 - beta_two) * (row_sum / n_total)
    c_new = beta_two * c_loc + (1.0 - beta_two) * (col_sum / m_total)
    r_mean = lax.psum(jnp.sum(r_new), 'row') / m_total
    update = grad_loc * lax.rsqrt(r_new[:, None] * c_new[None, :] / r_mean)
    u_sq = lax.psum(jnp.sum(update * update), ('row', 'col'))
    rms_u = jnp.sqrt(u_sq / (m_total * n_total))
    update_hat = update / jnp.maximum(1.0, rms_u / hyper_params[2])
    w_sq = lax.psum(jnp.sum(w_loc * w_loc), ('row', 'col'))
    step_size = hyper_params[1] * jnp.maximum(EPS_TWO, jnp.sqrt(w_sq / (m_total * n_total)))
    return w_loc - step_size * update_hat, r_new, c_new


def weight_grad(activations, grad_out):
    return lax.dot_general(activations, grad_out, (((0,), (0,)), ((), ())), preferred_element_type=jnp.float32)


def solution(mesh):
    row_size = mesh.shape['row']
    col_size = mesh.shape['col']
    weight_spec = P('row', 'col')
    act_spec = P(None, 'row')
    grad_spec = P(None, 'col')
    in_specs = (weight_spec,) * 3 + (act_spec, act_spec) + (grad_spec,) * 3 + (P('row'), P('col')) * 3 + (P(),)
    out_specs = (weight_spec,) * 3 + (P('row'), P('col')) * 3 + (act_spec, act_spec)

    def body(w_gate, w_up, w_down, x_norm, x_act, dy_gate, dy_up, dy_down, r_gate, c_gate, r_up, c_up, r_down, c_down, hyper_params):
        d_model = w_gate.shape[0] * row_size
        d_ff = w_gate.shape[1] * col_size
        dy = jnp.concatenate([dy_gate, dy_up, dy_down], axis=1)
        wn = jnp.concatenate([w_gate.astype(BF16).T, w_up.astype(BF16).T], axis=0)
        wa = w_down.astype(BF16).T
        dxn, dxa = exchange(dy, wn, wa)
        dxn, dxa, x_norm, x_act = lax.optimization_barrier((dxn, dxa, x_norm, x_act))
        dx_act = lax.all_gather(dxa, 'col', axis=0, tiled=True)
        dx_norm = lax.all_gather(dxn, 'col', axis=0, tiled=True)
        new_gate, r_gate_new, c_gate_new = factored_step(w_gate, weight_grad(x_norm, dy_gate), r_gate, c_gate, hyper_params, d_model, d_ff)
        new_up, r_up_new, c_up_new = factored_step(w_up, weight_grad(x_norm, dy_up), r_up, c_up, hyper_params, d_model, d_ff)
        new_down, r_down_new, c_down_new = factored_step(w_down, weight_grad(x_act, dy_down), r_down, c_down, hyper_params, d_ff, d_model)
        return (new_gate, new_up, new_down, r_gate_new, c_gate_new, r_up_new, c_up_new, r_down_new, c_down_new, dx_norm, dx_act)

    return jax.shard_map(body, mesh=mesh, in_specs=in_specs, out_specs=out_specs, check_vma=False)
```

```python
import jax
import jax.numpy as jnp
from jax import lax
from jax.experimental import pallas as pl
from jax.experimental.pallas import tpu as pltpu
from jax.sharding import PartitionSpec as P

EPS_ONE = 1e-30
EPS_TWO = 1e-3
MESH = pl.DeviceIdType.MESH
NY, NZ, NX = 4, 8, 4
NCOL, NROW = NY * NZ, NX * 2
LONG = NCOL // 2
BF16, F32 = jnp.bfloat16, jnp.float32


def ring_place(cycle, col):
    y, z = col % NY, col // NY
    u = (y + z) % NY
    if cycle == 0:
        return NY * z + u
    return NY * ((3 * (z - u + NZ)) % NZ) + u


def ring_col(cycle, place):
    place = (place + NCOL) % NCOL
    q, u = place // NY, place % NY
    z = q if cycle == 0 else (3 * q + u) % NZ
    return z * NY + (u - z + NZ) % NY


class Rings:
    def __init__(self, col, row, parts, send_sems, recv_sems):
        self.row, self.parts, self.send_sems, self.recv_sems = row, parts, send_sems, recv_sems
        sign = 1 - 2 * (row % 2)
        self.lanes = []
        for cycle in range(2):
            place = ring_place(cycle, col)
            for way in range(2):
                step_dir = sign if way == 0 else -sign
                self.lanes.append((cycle, way, place, step_dir, ring_col(cycle, place + step_dir)))

    def copy(self, lane, step, k):
        cycle, way, place, step_dir, peer = self.lanes[lane]
        ref = self.parts[k](cycle, ring_col(cycle, place - step_dir * step))
        return pltpu.make_async_remote_copy(
            src_ref=ref, dst_ref=ref, send_sem=self.send_sems.at[lane, k], recv_sem=self.recv_sems.at[lane, step, k],
            device_id=(peer, self.row), device_id_type=MESH)

    def start(self, step):
        for k in range(len(self.parts)):
            for lane in range(4):
                self.guard(lane, step, lambda lane=lane, k=k: self.copy(lane, step, k).start())

    def guard(self, lane, step, go):
        n_steps = LONG - self.lanes[lane][1]
        if isinstance(step, int):
            if step < n_steps:
                go()
        else:
            pl.when(step < n_steps)(go)

    def wait_recv(self, step):
        for k in range(len(self.parts)):
            for lane in range(4):
                self.guard(lane, step, lambda lane=lane, k=k: self.copy(lane, step, k).wait_recv())

    def forward(self, step):
        for k in range(len(self.parts)):
            for lane in range(4):
                self.guard(lane, step - 1, lambda lane=lane, k=k: self.copy(lane, step - 1, k).wait_recv())
                self.guard(lane, step, lambda lane=lane, k=k: self.copy(lane, step, k).start())

    def wait_sends(self, totals):
        for lane in range(4):
            for k, total in enumerate(totals):
                ref = total(LONG - self.lanes[lane][1])
                pltpu.make_async_copy(ref, ref, self.send_sems.at[lane, k]).wait()


def step_kernel(dyg_ref, dyu_ref, dyd_ref, xn_ref, xa_ref, wn_ref, wa_ref, wg_ref, wu_ref, wd_ref, r_ref, c_ref, hyper_ref,
                wg_out, wu_out, wd_out, r_out, c_out, dxn_ref, dxa_ref,
                dn_all, dd_all, wn_all, wa_all, acc_n, acc_a, own_n, own_a,
                xn_buf, xa_buf, dyn_buf, dyd_buf, grad_n, grad_d,
                col_msg, row_msg, u_msg, r_msg, z_msg,
                w_send, w_recv, ag_send, ag_recv, local_sem, a2a_sems, x_send, x_recv, tile_sems, st_send, st_recv):
    col, row = lax.axis_index('col'), lax.axis_index('row')
    x, core = row // 2, row % 2
    tokens = dxn_ref.shape[0] // NCOL
    quarter = tokens // NX
    ng = dyg_ref.shape[0]
    nd = dyd_ref.shape[0]
    nn = 2 * ng
    hd = nd // 2
    fetch_own = [pltpu.make_async_copy(wn_ref, wn_all.at[col], local_sem.at[0]),
                 pltpu.make_async_copy(wa_ref, wa_all.at[col], local_sem.at[1])]

    w_rings = Rings(col, row, [
        lambda cycle, origin: wn_all.at[origin, pl.ds(cycle * ng, ng)],
        lambda cycle, origin: wa_all.at[origin, pl.ds(cycle * hd, hd)]], w_send, w_recv)
    if DO_W:
        for copy in fetch_own:
            copy.start()
        for copy in fetch_own:
            copy.wait()
        w_rings.start(0)

    rows_n, rows_d = pl.ds(core * ng, ng), pl.ds(core * hd, hd)

    def a2a(src):
        @pl.loop(0, NCOL)
        def _(shift):
            peer = (col + shift) % NCOL
            cols = pl.ds(pl.multiple_of(peer * tokens + x * quarter, quarter), quarter)
            pieces = ((src.at[:, cols], dn_all.at[x, col, rows_n]), (dyd_ref.at[rows_d, cols], dd_all.at[x, col, rows_d]))

            @pl.when(shift == 0)
            def _():
                for k, (s, d) in enumerate(pieces):
                    pltpu.make_async_copy(s, d, a2a_sems.at[1, k]).start()

            @pl.when(shift > 0)
            def _():
                for k, (s, d) in enumerate(pieces):
                    pltpu.make_async_remote_copy(src_ref=s, dst_ref=d, send_sem=a2a_sems.at[0, k], recv_sem=a2a_sems.at[1, k],
                                                 device_id=(peer, row), device_id_type=MESH).start()

    if DO_A2A:
        pl.when(core == 0)(lambda: a2a(dyg_ref))
        pl.when(core == 1)(lambda: a2a(dyu_ref))

    def x_of(dx):
        return (x + dx + NX) % NX

    half = NCOL // 2
    every, low, high = pl.ds(0, NCOL), pl.ds(0, half), pl.ds(half, half)
    own, prev, succ, far = x, x_of(-1), x_of(1), x_of(2)
    partner = x * 2 + 1 - core

    class Hop:
        def __init__(self, k, slot, target, cols=every):
            refs = (dn_all.at[slot, cols, rows_n], dd_all.at[slot, cols, rows_d])
            self.copies = [pltpu.make_async_remote_copy(
                src_ref=ref, dst_ref=ref, send_sem=x_send.at[k, p], recv_sem=x_recv.at[k, p],
                device_id=(col, target), device_id_type=MESH) for p, ref in enumerate(refs)]

        def start(self):
            for copy in self.copies:
                copy.start()

        def wait_recv(self):
            for copy in self.copies:
                copy.wait_recv()

        def wait_send(self):
            for copy in self.copies:
                copy.wait_send()

    to_succ, to_prev = succ * 2 + core, prev * 2 + core
    hops = [
        Hop(0, own, to_succ), Hop(1, own, to_prev), Hop(2, own, partner),
        Hop(3, prev, to_succ, low), Hop(4, prev, partner),
        Hop(5, succ, to_prev, high), Hop(6, succ, partner),
        Hop(7, far, partner, low), Hop(8, far, partner, high)]

    def w_steps(first, last):
        if DO_W:
            @pl.loop(first, last)
            def _(step):
                w_rings.forward(step)

    w_steps(1, W_A)
    if DO_A2A:
        for k, ref in enumerate((dn_all.at[x, every, rows_n], dd_all.at[x, every, rows_d])):
            pltpu.make_async_copy(ref, ref, a2a_sems.at[1, k]).wait()
    if DO_X:
        for k in (0, 1, 2):
            hops[k].start()
    w_steps(W_A, W_B)
    if DO_X:
        hops[0].wait_recv()
        hops[3].start()
        hops[4].start()
        hops[1].wait_recv()
        hops[5].start()
        hops[6].start()
    w_steps(W_B, LONG)
    if DO_W:
        w_rings.wait_recv(LONG - 1)
    if DO_X:
        hops[3].wait_recv()
        hops[7].start()
        hops[5].wait_recv()
        hops[8].start()
        for k in (2, 4, 6, 7, 8):
            hops[k].wait_recv()

    group = 4
    if DO_MM:
        @pl.loop(0, NCOL // group)
        def _(g):
            js = pl.ds(g * group, group)
            lhs_n = jnp.concatenate([dn_all[q, js].reshape(group * nn, quarter) for q in range(NX)], axis=1)
            lhs_d = jnp.concatenate([dd_all[q, js].reshape(group * nd, quarter) for q in range(NX)], axis=1)
            dims = (((0,), (0,)), ((), ()))
            part_n = lax.dot_general(lhs_n, wn_all[js].reshape(group * nn, wn_all.shape[2]), dims, preferred_element_type=F32)
            part_a = lax.dot_general(lhs_d, wa_all[js].reshape(group * nd, wa_all.shape[2]), dims, preferred_element_type=F32)

            @pl.when(g == 0)
            def _():
                acc_n[...] = part_n
                acc_a[...] = part_a

            @pl.when(g > 0)
            def _():
                acc_n[...] += part_n
                acc_a[...] += part_a

    own_n[...] = acc_n[...].astype(BF16)
    own_a[...] = acc_a[...].astype(BF16)
    mine = pl.ds(pl.multiple_of(col * tokens, tokens), tokens)
    place_own = [pltpu.make_async_copy(own_n, dxn_ref.at[mine], local_sem.at[0]),
                 pltpu.make_async_copy(own_a, dxa_ref.at[mine], local_sem.at[1])]
    for copy in place_own:
        copy.start()
    for copy in place_own:
        copy.wait()

    def span(ref, offset, count):
        def part(cycle, origin):
            return ref.at[pl.ds(pl.multiple_of(origin * tokens + cycle * (tokens // 2) + offset, 16), count)]
        return part

    sizes = [(dxa_ref, tokens // 4), (dxa_ref, tokens // 4), (dxn_ref, tokens // 2)]
    ag = Rings(col, row, [span(dxa_ref, 0, tokens // 4), span(dxa_ref, tokens // 4, tokens // 4), span(dxn_ref, 0, tokens // 2)],
               ag_send, ag_recv)

    tile = xn_buf.shape[1]
    n_tiles = dxn_ref.shape[0] // tile

    def tile_copies(t, slot):
        at = pl.ds(pl.multiple_of(t * tile, tile), tile)
        pairs = ((xn_ref.at[at], xn_buf.at[slot]), (xa_ref.at[at], xa_buf.at[slot]),
                 (dyg_ref.at[:, at], dyn_buf.at[slot, pl.ds(0, ng)]), (dyu_ref.at[:, at], dyn_buf.at[slot, pl.ds(ng, ng)]),
                 (dyd_ref.at[:, at], dyd_buf.at[slot]))
        return [pltpu.make_async_copy(s, d, tile_sems.at[slot, k]) for k, (s, d) in enumerate(pairs)]

    def dw_tile(t):
        slot = t % 2
        for copy in tile_copies(t, slot):
            copy.wait()

        @pl.when(t + 1 < n_tiles)
        def _():
            for copy in tile_copies(t + 1, 1 - slot):
                copy.start()
        grad_n[...] += jnp.dot(dyn_buf[slot], xn_buf[slot], preferred_element_type=F32)
        grad_d[...] += jnp.dot(dyd_buf[slot], xa_buf[slot], preferred_element_type=F32)

    if DO_AG:
        ag.start(0)
    grad_n[...] = jnp.zeros_like(grad_n)
    grad_d[...] = jnp.zeros_like(grad_d)
    if DO_DW:
        for copy in tile_copies(0, 0):
            copy.start()
    per_step = n_tiles // DW_STEPS

    @pl.loop(1, DW_STEPS + 1)
    def _(step):
        if DO_AG:
            ag.forward(step)
        if DO_DW:
            @pl.loop(0, per_step)
            def _(k):
                dw_tile((step - 1) * per_step + k)

    def ag_step(step):
        if DO_AG:
            ag.forward(step)

    m = xn_ref.shape[1]
    beta_two, rho, clip = hyper_ref[0], hyper_ref[1], hyper_ref[2]
    n_elem = float(m * NROW * ng * NCOL)
    n_rows, n_cols = float(m * NROW), float(ng * NCOL)
    scales = ((n_rows, n_cols), (n_rows, n_cols), (n_cols, n_rows))

    def lanes_of(values):
        lane = lax.broadcasted_iota(jnp.int32, (1, 128), 1)
        out = jnp.zeros((1, 128), F32)
        for k, value in enumerate(values):
            out = jnp.where(lane == k, value, out)
        return out

    def scatter(k, ref, axis):
        count, mine_at = (NCOL, col) if axis == 'col' else (NROW, row)

        @pl.loop(1, count)
        def _(shift):
            peer = (mine_at + shift) % count
            target = (peer, row) if axis == 'col' else (col, peer)
            pltpu.make_async_remote_copy(src_ref=ref.at[mine_at], dst_ref=ref.at[mine_at], send_sem=st_send.at[k],
                                         recv_sem=st_recv.at[k], device_id=target, device_id_type=MESH).start()

    def collect(k, ref, count):
        part = ref.at[pl.ds(0, count - 1)]
        pltpu.make_async_copy(part, part, st_recv.at[k]).wait()

    def drain(k, ref, count):
        part = ref.at[pl.ds(0, count - 1)]
        pltpu.make_async_copy(part, part, st_send.at[k]).wait()

    def pick(vec, k):
        lane = lax.broadcasted_iota(jnp.int32, (1, 128), 1)
        return jnp.sum(jnp.where(lane == k, vec, 0.0))

    def grads():
        return grad_n[pl.ds(0, ng), :], grad_n[pl.ds(ng, ng), :], grad_d[...]

    ag_step(DW_STEPS + 1)
    squares = [g * g + EPS_ONE for g in grads()]
    w_parts = [jnp.sum(w[...] * w[...]) for w in (wg_ref, wu_ref, wd_ref)]
    row_sums = [jnp.sum(s, axis=0, keepdims=True) for s in squares]
    col_sums = jnp.concatenate([jnp.sum(s, axis=1, keepdims=True) for s in squares], axis=0)
    col_msg[col] = jnp.concatenate(row_sums + [lanes_of(w_parts)], axis=1)
    row_msg[row] = jnp.transpose(jnp.broadcast_to(col_sums, (nn + nd, 128)))[0:1, :]
    if DO_ST:
        scatter(0, col_msg, 'col')
        scatter(1, row_msg, 'row')

    ag_step(DW_STEPS + 2)
    if DO_ST:
        collect(0, col_msg, NCOL)
        collect(1, row_msg, NROW)
    r_total = jnp.sum(col_msg[...], axis=0)
    c_total = jnp.sum(row_msg[...], axis=0)
    n_r = r_total.shape[1] - 128
    lane_r = lax.broadcasted_iota(jnp.int32, (1, n_r), 1)
    lane_c = lax.broadcasted_iota(jnp.int32, (1, nn + nd), 1)
    r_new = beta_two * r_ref[...] + (1.0 - beta_two) * (r_total[:, :n_r] / jnp.where(lane_r < 2 * m, n_cols, n_rows))
    c_new = beta_two * c_ref[...] + (1.0 - beta_two) * (c_total / jnp.where(lane_c < nn, n_rows, n_cols))
    r_out[...] = r_new
    c_out[...] = c_new
    r_cuts = ((0, m), (m, 2 * m), (2 * m, n_r))
    r_sums = [jnp.sum(r_new[:, a:b]) for a, b in r_cuts]
    w_line = [pick(r_total[:, n_r:], k) for k in range(3)]
    r_msg[row] = lanes_of(r_sums + w_line)
    if DO_ST:
        scatter(2, r_msg, 'row')

    ag_step(DW_STEPS + 3)
    if DO_ST:
        collect(2, r_msg, NROW)
    totals = jnp.sum(r_msg[...], axis=0)
    c_col = jnp.transpose(jnp.broadcast_to(c_out[...], (128, nn + nd)))[:, 0:1]
    c_cols = (c_col[:ng], c_col[ng:nn], c_col[nn:])
    u_sums = []
    new_refs = (wg_out, wu_out, wd_out)
    for k, g in enumerate(grads()):
        r_mean = pick(totals, k) / scales[k][0]
        r_row = r_out[:, r_cuts[k][0]:r_cuts[k][1]]
        update = g * lax.rsqrt(r_row * c_cols[k] / r_mean)
        new_refs[k][...] = update
        u_sums.append(jnp.sum(update * update))
    w_sq = [pick(totals, 3 + k) for k in range(3)]
    u_msg[row] = lanes_of(u_sums)
    if DO_ST:
        scatter(3, u_msg, 'row')

    ag_step(DW_STEPS + 4)
    if DO_ST:
        collect(3, u_msg, NROW)
    z_msg[col] = jnp.sum(u_msg[...], axis=0)
    if DO_ST:
        scatter(4, z_msg, 'col')

    ag_step(DW_STEPS + 5)
    if DO_ST:
        collect(4, z_msg, NCOL)
    u_total = jnp.sum(z_msg[...], axis=0)

    def rms(value):
        return jnp.sqrt(jnp.full((1, 1), value / n_elem, F32))

    for k, (w, out) in enumerate(zip((wg_ref, wu_ref, wd_ref), new_refs)):
        shrink = jnp.maximum(1.0, rms(pick(u_total, k)) / clip)
        step_size = rho * jnp.maximum(EPS_TWO, rms(w_sq[k]))
        out[...] = w[...] - step_size * (out[...] / shrink)

    @pl.loop(DW_STEPS + 6, LONG)
    def _(step):
        ag_step(step)
    if DO_AG:
        ag.wait_recv(LONG - 1)

    if DO_X:
        for hop in hops:
            hop.wait_send()
    if DO_A2A:
        for k, ref in enumerate((dn_all.at[0, pl.ds(0, NCOL - 1), pl.ds(0, ng)], dd_all.at[0, pl.ds(0, NCOL - 1), pl.ds(0, hd)])):
            pltpu.make_async_copy(ref, ref, a2a_sems.at[0, k]).wait()
    if DO_W:
        w_rings.wait_sends([lambda n: wn_all.at[pl.ds(0, n), pl.ds(0, ng)], lambda n: wa_all.at[pl.ds(0, n), pl.ds(0, hd)]])
    if DO_AG:
        ag.wait_sends([lambda n, ref=ref, size=size: ref.at[pl.ds(0, n * size)] for ref, size in sizes])
    if DO_ST:
        for k, ref, count in ((0, col_msg, NCOL), (1, row_msg, NROW), (2, r_msg, NROW), (3, u_msg, NROW), (4, z_msg, NCOL)):
            drain(k, ref, count)


DO_W = DO_A2A = DO_X = DO_MM = DO_AG = DO_DW = DO_ST = True
W_A, W_B, DW_STEPS = 6, 11, 8
TILE = 512


def fused_step(dyg, dyu, dyd, xn, xa, wn, wa, wg, wu, wd, r_all, c_all, hyper):
    tokens = xn.shape[0] // NCOL
    ng, nd, m, ma = dyg.shape[0], dyd.shape[0], xn.shape[1], xa.shape[1]
    nn = 2 * ng
    vmem, hbm = pl.BlockSpec(memory_space=pltpu.VMEM), pl.BlockSpec(memory_space=pl.ANY)
    smem = pl.BlockSpec(memory_space=pltpu.SMEM)
    dma = pltpu.SemaphoreType.DMA
    shape = jax.ShapeDtypeStruct
    return pl.pallas_call(
        step_kernel,
        out_shape=(shape(wg.shape, F32), shape(wu.shape, F32), shape(wd.shape, F32), shape(r_all.shape, F32), shape(c_all.shape, F32),
                   shape(xn.shape, BF16), shape(xa.shape, BF16)),
        in_specs=[hbm] * 5 + [vmem] * 7 + [smem],
        out_specs=(vmem,) * 5 + (hbm,) * 2,
        scratch_shapes=[
            pltpu.VMEM((NX, NCOL, nn, tokens // NX), BF16),
            pltpu.VMEM((NX, NCOL, nd, tokens // NX), BF16),
            pltpu.VMEM((NCOL, nn, m), BF16),
            pltpu.VMEM((NCOL, nd, ma), BF16),
            pltpu.VMEM((tokens, m), F32),
            pltpu.VMEM((tokens, ma), F32),
            pltpu.VMEM((tokens, m), BF16),
            pltpu.VMEM((tokens, ma), BF16),
            pltpu.VMEM((2, TILE, m), BF16),
            pltpu.VMEM((2, TILE, ma), BF16),
            pltpu.VMEM((2, nn, TILE), BF16),
            pltpu.VMEM((2, nd, TILE), BF16),
            pltpu.VMEM((nn, m), F32),
            pltpu.VMEM((nd, ma), F32),
            pltpu.VMEM((NCOL, 1, 2 * m + ma + 128), F32),
            pltpu.VMEM((NROW, 1, nn + nd), F32),
            pltpu.VMEM((NROW, 1, 128), F32),
            pltpu.VMEM((NROW, 1, 128), F32),
            pltpu.VMEM((NCOL, 1, 128), F32),
            dma((4, 2)), dma((4, LONG, 2)), dma((4, 3)), dma((4, LONG, 3)), dma((2,)), dma((2, 2)), dma((9, 2)), dma((9, 2)),
            dma((2, 5)), dma((5,)), dma((5,)),
        ],
        compiler_params=pltpu.CompilerParams(has_side_effects=True, vmem_limit_bytes=60 * 1024 * 1024),
        name='fused_step',
    )(dyg, dyu, dyd, xn, xa, wn, wa, wg, wu, wd, r_all, c_all, hyper)


def solution(mesh):
    weight_spec = P('row', 'col')
    act_spec = P(None, 'row')
    grad_spec = P(None, 'col')
    in_specs = (weight_spec,) * 3 + (act_spec, act_spec) + (grad_spec,) * 3 + (P('row'), P('col')) * 3 + (P(),)
    out_specs = (weight_spec,) * 3 + (P('row'), P('col')) * 3 + (act_spec, act_spec)

    def body(w_gate, w_up, w_down, x_norm, x_act, dy_gate, dy_up, dy_down, r_gate, c_gate, r_up, c_up, r_down, c_down, hyper_params):
        m, ng = w_gate.shape
        wg, wu, wd = w_gate.T, w_up.T, w_down.T
        wn = jnp.concatenate([wg.astype(BF16), wu.astype(BF16)], axis=0)
        wa = wd.astype(BF16)
        r_all = jnp.concatenate([r_gate, r_up, r_down])[None]
        c_all = jnp.concatenate([c_gate, c_up, c_down])[None]
        wg, wu, wd, r_all, c_all, dx_norm, dx_act = fused_step(
            dy_gate.T, dy_up.T, dy_down.T, x_norm, x_act, wn, wa, wg, wu, wd, r_all, c_all, hyper_params)
        r_all, c_all = r_all[0], c_all[0]
        return (wg.T, wu.T, wd.T, r_all[:m], c_all[:ng], r_all[m:2 * m], c_all[ng:2 * ng], r_all[2 * m:], c_all[2 * ng:],
                dx_norm, dx_act)

    return jax.shard_map(body, mesh=mesh, in_specs=in_specs, out_specs=out_specs, check_vma=False)
```

```python
import jax
import jax.numpy as jnp
from jax import lax
from jax.experimental import pallas as pl
from jax.experimental.pallas import tpu as pltpu
from jax.sharding import PartitionSpec as P

EPS_ONE = 1e-30
EPS_TWO = 1e-3
MESH = pl.DeviceIdType.MESH
NY, NZ, NX = 4, 8, 4
NCOL, NROW = NY * NZ, NX * 2
LONG = NCOL // 2
BF16, F32 = jnp.bfloat16, jnp.float32


def ring_place(cycle, col):
    y, z = col % NY, col // NY
    u = (y + z) % NY
    if cycle == 0:
        return NY * z + u
    return NY * ((3 * (z - u + NZ)) % NZ) + u


def ring_col(cycle, place):
    place = (place + NCOL) % NCOL
    q, u = place // NY, place % NY
    z = q if cycle == 0 else (3 * q + u) % NZ
    return z * NY + (u - z + NZ) % NY


class Rings:
    def __init__(self, col, row, parts, send_sems, recv_sems):
        self.row, self.parts, self.send_sems, self.recv_sems = row, parts, send_sems, recv_sems
        sign = 1 - 2 * (row % 2)
        self.lanes = []
        for cycle in range(2):
            place = ring_place(cycle, col)
            for way in range(2):
                step_dir = sign if way == 0 else -sign
                self.lanes.append((cycle, way, place, step_dir, ring_col(cycle, place + step_dir)))

    def copy(self, lane, step, k):
        cycle, way, place, step_dir, peer = self.lanes[lane]
        ref = self.parts[k](cycle, ring_col(cycle, place - step_dir * step))
        return pltpu.make_async_remote_copy(
            src_ref=ref, dst_ref=ref, send_sem=self.send_sems.at[lane, k], recv_sem=self.recv_sems.at[lane, step, k],
            device_id=(peer, self.row), device_id_type=MESH)

    def start(self, step):
        for k in range(len(self.parts)):
            for lane in range(4):
                self.guard(lane, step, lambda lane=lane, k=k: self.copy(lane, step, k).start())

    def guard(self, lane, step, go):
        n_steps = LONG - self.lanes[lane][1]
        if isinstance(step, int):
            if step < n_steps:
                go()
        else:
            pl.when(step < n_steps)(go)

    def wait_recv(self, step):
        for k in range(len(self.parts)):
            for lane in range(4):
                self.guard(lane, step, lambda lane=lane, k=k: self.copy(lane, step, k).wait_recv())

    def forward(self, step):
        for k in range(len(self.parts)):
            for lane in range(4):
                self.guard(lane, step - 1, lambda lane=lane, k=k: self.copy(lane, step - 1, k).wait_recv())
                self.guard(lane, step, lambda lane=lane, k=k: self.copy(lane, step, k).start())

    def wait_sends(self, totals):
        for lane in range(4):
            for k, total in enumerate(totals):
                ref = total(LONG - self.lanes[lane][1])
                pltpu.make_async_copy(ref, ref, self.send_sems.at[lane, k]).wait()


class Trees:
    def __init__(self, col, row, pieces, send_sems, recv_sems):
        self.row, self.pieces, self.send_sems, self.recv_sems = row, pieces, send_sems, recv_sems
        self.y, self.z, self.sign = col % NY, col // NY, 1 - 2 * (row % 2)

    def at(self, dy, dz):
        y = (self.y + self.sign * dy + NY) % NY
        z = (self.z + self.sign * dz + NZ) % NZ
        return z * NY + y

    def copy(self, tree, k, origin, target):
        (ey, ez), (fy, fz) = origin, target
        ref = self.pieces[tree][k](self.at(ey, ez))
        return pltpu.make_async_remote_copy(
            src_ref=ref, dst_ref=ref, send_sem=self.send_sems.at[tree, k],
            recv_sem=self.recv_sems.at[tree, (ey - fy) % NY, (ez - fz) % NZ, k],
            device_id=(self.at(fy, fz), self.row), device_id_type=MESH)

    @staticmethod
    def children(tree, ey, ez):
        along_y = {0: [(1, (0, 1)), (-1, (0, 1))], -1: [(1, (0,))], 1: [(-1, (1,))], 2: []}[ey]
        if ez == 0:
            along_z = [1, -1]
        elif ez < 0:
            along_z = [1] if ez > -NZ // 2 else []
        else:
            along_z = [-1] if ez < NZ // 2 - 1 else []
        if tree == 0:
            ys, zs = (along_y if ez == 0 else []), along_z
        else:
            ys, zs = along_y, (along_z if ey == 0 else [])
        return [((0, f), (0, 1)) for f in zs] + [((f, 0), ks) for f, ks in ys]

    def wait(self, tree, k, ey, ez):
        ref = self.pieces[tree][k](self.at(ey, ez))
        pltpu.make_async_copy(ref, ref, self.recv_sems.at[tree, ey % NY, ez % NZ, k]).wait()

    def round(self, r):
        for tree in (1, 0):
            for ez in (0, -1, 1, -2, 2, -3, 3, -4):
                for ey in (0, -1, 1, 2):
                    if abs(ey) + abs(ez) != r:
                        continue
                    if r:
                        for k in range(2):
                            self.wait(tree, k, ey, ez)
                    for target, ks in self.children(tree, ey, ez):
                        for k in ks:
                            self.copy(tree, k, (ey, ez), target).start()


def step_kernel(dyg_ref, dyu_ref, dyd_ref, xn_ref, xa_ref, wn_ref, wa_ref, wg_ref, wu_ref, wd_ref, r_ref, c_ref, hyper_ref,
                wg_out, wu_out, wd_out, r_out, c_out, dxn_ref, dxa_ref,
                dn_all, dd_all, wn_all, wa_all, acc_n, acc_a,
                xn_buf, xa_buf, dyn_buf, dyd_buf, grad_n, grad_d,
                col_msg, row_msg, u_msg, r_msg, z_msg,
                w_send, w_recv, ag_send, ag_recv, local_sem, a2a_sent, a2a_recv, x_send, x_recv, tile_sems, st_send, st_recv):
    col, row = lax.axis_index('col'), lax.axis_index('row')
    x, core = row // 2, row % 2
    tokens = dxn_ref.shape[0] // NCOL
    quarter = tokens // NX
    ng = dyg_ref.shape[0]
    nd = dyd_ref.shape[0]
    nn = 2 * ng
    hd = nd // 2
    fetch_own = [pltpu.make_async_copy(wn_ref, wn_all.at[col], local_sem.at[0]),
                 pltpu.make_async_copy(wa_ref, wa_all.at[col], local_sem.at[1])]

    def w_piece(ref, first, count):
        return lambda origin: ref.at[origin, pl.ds(first, count)]

    w_cuts = (((wn_all, 0, W_CUT), (wa_all, 0, hd)), ((wn_all, W_CUT, nn - W_CUT), (wa_all, hd, hd)))
    trees = Trees(col, row, [[w_piece(*cut) for cut in cuts] for cuts in w_cuts], w_send, w_recv)

    rows_n, rows_d = pl.ds(core * ng, ng), pl.ds(core * hd, hd)

    def shift_of(t):
        return ((2 * (t % 2) - 1) * ((t + 1) // 2) + NCOL) % NCOL

    def a2a_pieces(src, t, peer):
        cols = pl.ds(pl.multiple_of(peer * tokens + x * quarter, quarter), quarter)
        return (src.at[:, cols], dn_all.at[x, t, rows_n]), (dyd_ref.at[rows_d, cols], dd_all.at[x, t, rows_d])

    def a2a_own(src):
        for k, (s, d) in enumerate(a2a_pieces(src, 0, col)):
            pltpu.make_async_copy(s, d, a2a_recv.at[0, k]).start()

    def a2a_send(src, first, last):
        @pl.loop(first, last)
        def _(t):
            peer = (col + shift_of(t)) % NCOL
            for k, (s, d) in enumerate(a2a_pieces(src, t, peer)):
                pltpu.make_async_remote_copy(src_ref=s, dst_ref=d, send_sem=a2a_sent.at[k], recv_sem=a2a_recv.at[t // CHUNK, k],
                                             device_id=(peer, row), device_id_type=MESH).start()

    def by_core(go, *args):
        pl.when(core == 0)(lambda: go(dyg_ref, *args))
        pl.when(core == 1)(lambda: go(dyu_ref, *args))

    def x_of(dx):
        return (x + dx + NX) % NX

    own, prev, succ, far = x, x_of(-1), x_of(1), x_of(2)
    partner = x * 2 + 1 - core
    to_succ, to_prev = succ * 2 + core, prev * 2 + core
    routes = ((own, to_succ, 0, 2), (own, to_prev, 0, 2), (own, partner, 0, 2), (prev, to_succ, 0, 1), (prev, partner, 0, 2),
              (succ, to_prev, 1, 1), (succ, partner, 0, 2), (far, partner, 0, 1), (far, partner, 1, 1))

    def hop(k, ch):
        slot, target, first, count = routes[k]
        cols = pl.ds(ch * CHUNK + first * (CHUNK // 2), count * (CHUNK // 2))
        refs = (dn_all.at[slot, cols, rows_n], dd_all.at[slot, cols, rows_d])
        return [pltpu.make_async_remote_copy(
            src_ref=ref, dst_ref=ref, send_sem=x_send.at[k, ch, p], recv_sem=x_recv.at[k, ch, p],
            device_id=(col, target), device_id_type=MESH) for p, ref in enumerate(refs)]

    def hop_start(ch, *ks):
        for k in ks:
            for copy in hop(k, ch):
                copy.start()

    def hop_wait(ch, *ks):
        for k in ks:
            for copy in hop(k, ch):
                copy.wait_recv()

    def x_first(ch):
        cols = pl.ds(ch * CHUNK, CHUNK)
        for k, ref in enumerate((dn_all.at[x, cols, rows_n], dd_all.at[x, cols, rows_d])):
            pltpu.make_async_copy(ref, ref, a2a_recv.at[ch, k]).wait()
        if DO_X:
            hop_start(ch, 0, 1, 2)

    def x_second(ch):
        if DO_X:
            hop_wait(ch, 0)
            hop_start(ch, 3, 4)
            hop_wait(ch, 1)
            hop_start(ch, 5, 6)

    def x_third(ch):
        if DO_X:
            hop_wait(ch, 3)
            hop_start(ch, 7)
            hop_wait(ch, 5)
            hop_start(ch, 8)

    def x_last(ch):
        if DO_X:
            hop_wait(ch, 2, 4, 6, 7, 8)

    n_chunks = NCOL // CHUNK
    events = {}
    for ch in range(n_chunks):
        for stage, at in zip((x_first, x_second, x_third), X_AT[ch]):
            events.setdefault(at, []).append((stage, ch))

    if DO_W:
        for copy in fetch_own:
            copy.start()
    if DO_A2A:
        by_core(a2a_own)
    if DO_W:
        for copy in fetch_own:
            copy.wait()
    for r in range(ROUNDS + 1):
        if DO_W:
            trees.round(r)
        if DO_A2A:
            first, last = max(1, A2A_AT[r]), A2A_AT[r + 1]
            if first < last:
                by_core(a2a_send, first, last)
            for stage, ch in events.get(r, ()):
                stage(ch)

    group = 4
    for ch in range(n_chunks):
        if DO_A2A:
            for stage, late in events.get(ROUNDS + 1 + ch, ()):
                stage(late)
            x_last(ch)
        if DO_MM:
            @pl.loop(ch * (CHUNK // group), (ch + 1) * (CHUNK // group))
            def _(g):
                slots = pl.ds(g * group, group)
                js = [(col - shift_of(g * group + i) + NCOL) % NCOL for i in range(group)]
                lhs_n = jnp.concatenate([dn_all[q, slots].reshape(group * nn, quarter) for q in range(NX)], axis=1)
                lhs_d = jnp.concatenate([dd_all[q, slots].reshape(group * nd, quarter) for q in range(NX)], axis=1)
                dims = (((0,), (0,)), ((), ()))
                part_n = lax.dot_general(lhs_n, jnp.concatenate([wn_all[j] for j in js], axis=0), dims, preferred_element_type=F32)
                part_a = lax.dot_general(lhs_d, jnp.concatenate([wa_all[j] for j in js], axis=0), dims, preferred_element_type=F32)

                @pl.when(g == 0)
                def _():
                    acc_n[...] = part_n
                    acc_a[...] = part_a

                @pl.when(g > 0)
                def _():
                    acc_n[...] += part_n
                    acc_a[...] += part_a

    mine = pl.ds(pl.multiple_of(col * tokens, tokens), tokens)
    dxn_ref[mine, :] = acc_n[...].astype(BF16)
    dxa_ref[mine, :] = acc_a[...].astype(BF16)

    def span(ref, offset, count):
        def part(cycle, origin):
            return ref.at[pl.ds(pl.multiple_of(origin * tokens + cycle * (tokens // 2) + offset, 16), count)]
        return part

    sizes = [(dxa_ref, tokens // 4), (dxa_ref, tokens // 4), (dxn_ref, tokens // 2)]
    ag = Rings(col, row, [span(dxa_ref, 0, tokens // 4), span(dxa_ref, tokens // 4, tokens // 4), span(dxn_ref, 0, tokens // 2)],
               ag_send, ag_recv)

    tile = xn_buf.shape[1]
    n_tiles = dxn_ref.shape[0] // tile

    def tile_copies(t, slot):
        at = pl.ds(pl.multiple_of(t * tile, tile), tile)
        pairs = ((xn_ref.at[at], xn_buf.at[slot]), (xa_ref.at[at], xa_buf.at[slot]),
                 (dyg_ref.at[:, at], dyn_buf.at[slot, pl.ds(0, ng)]), (dyu_ref.at[:, at], dyn_buf.at[slot, pl.ds(ng, ng)]),
                 (dyd_ref.at[:, at], dyd_buf.at[slot]))
        return [pltpu.make_async_copy(s, d, tile_sems.at[slot, k]) for k, (s, d) in enumerate(pairs)]

    def dw_tile(t):
        slot = t % 2
        for copy in tile_copies(t, slot):
            copy.wait()

        @pl.when(t + 1 < n_tiles)
        def _():
            for copy in tile_copies(t + 1, 1 - slot):
                copy.start()
        grad_n[...] += jnp.dot(dyn_buf[slot], xn_buf[slot], preferred_element_type=F32)
        grad_d[...] += jnp.dot(dyd_buf[slot], xa_buf[slot], preferred_element_type=F32)

    if DO_DW:
        for copy in tile_copies(0, 0):
            copy.start()
    grad_n[...] = jnp.zeros_like(grad_n)
    grad_d[...] = jnp.zeros_like(grad_d)
    if DO_AG:
        ag.start(0)
    per_step = n_tiles // DW_STEPS

    @pl.loop(1, DW_STEPS + 1)
    def _(step):
        if DO_AG:
            ag.forward(step)
        if DO_DW:
            @pl.loop(0, per_step)
            def _(k):
                dw_tile((step - 1) * per_step + k)

    def ag_step(step):
        if DO_AG:
            ag.forward(step)

    m = xn_ref.shape[1]
    beta_two, rho, clip = hyper_ref[0], hyper_ref[1], hyper_ref[2]
    n_elem = float(m * NROW * ng * NCOL)
    n_rows, n_cols = float(m * NROW), float(ng * NCOL)
    scales = ((n_rows, n_cols), (n_rows, n_cols), (n_cols, n_rows))

    def lanes_of(values):
        lane = lax.broadcasted_iota(jnp.int32, (1, 128), 1)
        out = jnp.zeros((1, 128), F32)
        for k, value in enumerate(values):
            out = jnp.where(lane == k, value, out)
        return out

    def scatter(k, ref, axis):
        count, mine_at = (NCOL, col) if axis == 'col' else (NROW, row)

        @pl.loop(1, count)
        def _(shift):
            peer = (mine_at + shift) % count
            target = (peer, row) if axis == 'col' else (col, peer)
            pltpu.make_async_remote_copy(src_ref=ref.at[mine_at], dst_ref=ref.at[mine_at], send_sem=st_send.at[k],
                                         recv_sem=st_recv.at[k], device_id=target, device_id_type=MESH).start()

    def collect(k, ref, count):
        part = ref.at[pl.ds(0, count - 1)]
        pltpu.make_async_copy(part, part, st_recv.at[k]).wait()

    def drain(k, ref, count):
        part = ref.at[pl.ds(0, count - 1)]
        pltpu.make_async_copy(part, part, st_send.at[k]).wait()

    def pick(vec, k):
        lane = lax.broadcasted_iota(jnp.int32, (1, 128), 1)
        return jnp.sum(jnp.where(lane == k, vec, 0.0))

    def grads():
        return grad_n[pl.ds(0, ng), :], grad_n[pl.ds(ng, ng), :], grad_d[...]

    ag_step(DW_STEPS + 1)
    squares = [g * g + EPS_ONE for g in grads()]
    w_parts = [jnp.sum(w[...] * w[...]) for w in (wg_ref, wu_ref, wd_ref)]
    row_sums = [jnp.sum(s, axis=0, keepdims=True) for s in squares]
    col_sums = jnp.concatenate([jnp.sum(s, axis=1, keepdims=True) for s in squares], axis=0)
    col_msg[col] = jnp.concatenate(row_sums + [lanes_of(w_parts)], axis=1)
    row_msg[row] = jnp.transpose(jnp.broadcast_to(col_sums, (nn + nd, 128)))[0:1, :]
    if DO_ST:
        scatter(0, col_msg, 'col')
        scatter(1, row_msg, 'row')

    ag_step(DW_STEPS + 2)
    if DO_ST:
        collect(0, col_msg, NCOL)
        collect(1, row_msg, NROW)
    r_total = jnp.sum(col_msg[...], axis=0)
    c_total = jnp.sum(row_msg[...], axis=0)
    n_r = r_total.shape[1] - 128
    lane_r = lax.broadcasted_iota(jnp.int32, (1, n_r), 1)
    lane_c = lax.broadcasted_iota(jnp.int32, (1, nn + nd), 1)
    r_new = beta_two * r_ref[...] + (1.0 - beta_two) * (r_total[:, :n_r] / jnp.where(lane_r < 2 * m, n_cols, n_rows))
    c_new = beta_two * c_ref[...] + (1.0 - beta_two) * (c_total / jnp.where(lane_c < nn, n_rows, n_cols))
    r_out[...] = r_new
    c_out[...] = c_new
    r_cuts = ((0, m), (m, 2 * m), (2 * m, n_r))
    r_sums = [jnp.sum(r_new[:, a:b]) for a, b in r_cuts]
    w_line = [pick(r_total[:, n_r:], k) for k in range(3)]
    r_msg[row] = lanes_of(r_sums + w_line)
    if DO_ST:
        scatter(2, r_msg, 'row')

    ag_step(DW_STEPS + 3)
    if DO_ST:
        collect(2, r_msg, NROW)
    totals = jnp.sum(r_msg[...], axis=0)
    c_col = jnp.transpose(jnp.broadcast_to(c_out[...], (128, nn + nd)))[:, 0:1]
    c_cols = (c_col[:ng], c_col[ng:nn], c_col[nn:])
    u_sums = []
    new_refs = (wg_out, wu_out, wd_out)
    for k, g in enumerate(grads()):
        r_mean = pick(totals, k) / scales[k][0]
        r_row = r_out[:, r_cuts[k][0]:r_cuts[k][1]]
        update = g * lax.rsqrt(r_row * c_cols[k] / r_mean)
        new_refs[k][...] = update
        u_sums.append(jnp.sum(update * update))
    w_sq = [pick(totals, 3 + k) for k in range(3)]
    u_msg[row] = lanes_of(u_sums)
    if DO_ST:
        scatter(3, u_msg, 'row')

    ag_step(DW_STEPS + 4)
    if DO_ST:
        collect(3, u_msg, NROW)
    z_msg[col] = jnp.sum(u_msg[...], axis=0)
    if DO_ST:
        scatter(4, z_msg, 'col')

    ag_step(DW_STEPS + 5)
    if DO_ST:
        collect(4, z_msg, NCOL)
    u_total = jnp.sum(z_msg[...], axis=0)

    def rms(value):
        return jnp.sqrt(jnp.full((1, 1), value / n_elem, F32))

    for k, (w, out) in enumerate(zip((wg_ref, wu_ref, wd_ref), new_refs)):
        shrink = jnp.maximum(1.0, rms(pick(u_total, k)) / clip)
        step_size = rho * jnp.maximum(EPS_TWO, rms(w_sq[k]))
        out[...] = w[...] - step_size * (out[...] / shrink)

    @pl.loop(DW_STEPS + 6, LONG)
    def _(step):
        ag_step(step)
    if DO_AG:
        ag.wait_recv(LONG - 1)

    if DO_X:
        for ch in range(n_chunks):
            for k in range(len(routes)):
                for copy in hop(k, ch):
                    copy.wait_send()
    if DO_A2A:
        for k, ref in enumerate((dn_all.at[0, pl.ds(0, NCOL - 1), pl.ds(0, ng)], dd_all.at[0, pl.ds(0, NCOL - 1), pl.ds(0, hd)])):
            pltpu.make_async_copy(ref, ref, a2a_sent.at[k]).wait()
    if DO_W:
        for tree, cuts in enumerate(w_cuts):
            for k, (ref, _, count) in enumerate(cuts):
                ref = ref.at[pl.ds(0, NCOL - 1), pl.ds(0, count)]
                pltpu.make_async_copy(ref, ref, w_send.at[tree, k]).wait()
    if DO_AG:
        ag.wait_sends([lambda n, ref=ref, size=size: ref.at[pl.ds(0, n * size)] for ref, size in sizes])
    if DO_ST:
        for k, ref, count in ((0, col_msg, NCOL), (1, row_msg, NROW), (2, r_msg, NROW), (3, u_msg, NROW), (4, z_msg, NCOL)):
            drain(k, ref, count)


DO_W = DO_A2A = DO_X = DO_MM = DO_AG = DO_DW = DO_ST = True
CHUNK, DW_STEPS = 8, 8
ROUNDS = NY // 2 + NZ // 2
A2A_AT = (0, 8, 16, 24, 32, 32, 32, 32)
X_AT = ((1, 2, 3), (2, 3, 4), (3, 4, 5), (4, 5, 7))
W_CUT = 128
TILE = 512


VMEM_LIMIT = 33 * 1024 * 1024
PIECES = 8


def finish_kernel(wg_ref, wu_ref, wd_ref, r_ref, c_ref, dxn_ref, dxa_ref,
                  wg_out, wu_out, wd_out, rg_out, cg_out, ru_out, cu_out, rd_out, cd_out, dxn_out, dxa_out, sems):
    rows = dxn_ref.shape[0] // PIECES
    copies = [pltpu.make_async_copy(src.at[pl.ds(k * rows, rows)], dst.at[pl.ds(k * rows, rows)], sems.at[p, k])
              for p, (src, dst) in enumerate(((dxa_ref, dxa_out), (dxn_ref, dxn_out))) for k in range(PIECES)]
    for copy in copies:
        copy.start()
    for src, dst in ((wg_ref, wg_out), (wu_ref, wu_out), (wd_ref, wd_out)):
        dst[...] = src[...]
    for src, outs in ((r_ref, (rg_out, ru_out, rd_out)), (c_ref, (cg_out, cu_out, cd_out))):
        at = 0
        for out in outs:
            out[...] = src[:, at:at + out.shape[1]]
            at += out.shape[1]
    for copy in copies:
        copy.wait()


def finish(wg, wu, wd, r_all, c_all, dxn, dxa):
    vmem, hbm = pl.BlockSpec(memory_space=pltpu.VMEM), pl.BlockSpec(memory_space=pl.ANY)
    shape = jax.ShapeDtypeStruct
    ng, m = wg.shape
    nd, ma = wd.shape
    stats = [shape((1, n), F32) for n in (m, ng, m, ng, ma, nd)]
    return pl.pallas_call(
        finish_kernel,
        out_shape=[shape(w.shape, F32) for w in (wg, wu, wd)] + stats + [shape(dxn.shape, BF16), shape(dxa.shape, BF16)],
        in_specs=[vmem] * 7,
        out_specs=[vmem] * 9 + [hbm] * 2,
        scratch_shapes=[pltpu.SemaphoreType.DMA((2, PIECES))],
        compiler_params=pltpu.CompilerParams(vmem_limit_bytes=1 * 1024 * 1024),
        name='finish',
    )(wg, wu, wd, r_all, c_all, dxn, dxa)


def fused_step(dyg, dyu, dyd, xn, xa, wn, wa, wg, wu, wd, r_all, c_all, hyper):
    tokens = xn.shape[0] // NCOL
    ng, nd, m, ma = dyg.shape[0], dyd.shape[0], xn.shape[1], xa.shape[1]
    nn = 2 * ng
    vmem, hbm = pl.BlockSpec(memory_space=pltpu.VMEM), pl.BlockSpec(memory_space=pl.ANY)
    smem = pl.BlockSpec(memory_space=pltpu.SMEM)
    dma = pltpu.SemaphoreType.DMA
    shape = jax.ShapeDtypeStruct
    return pl.pallas_call(
        step_kernel,
        out_shape=(shape(wg.shape, F32), shape(wu.shape, F32), shape(wd.shape, F32), shape(r_all.shape, F32), shape(c_all.shape, F32),
                   pltpu.VMEM(xn.shape, BF16), pltpu.VMEM(xa.shape, BF16)),
        in_specs=[hbm] * 5 + [vmem] * 7 + [smem],
        out_specs=(vmem,) * 7,
        scratch_shapes=[
            pltpu.VMEM((NX, NCOL, nn, tokens // NX), BF16),
            pltpu.VMEM((NX, NCOL, nd, tokens // NX), BF16),
            pltpu.VMEM((NCOL, nn, m), BF16),
            pltpu.VMEM((NCOL, nd, ma), BF16),
            pltpu.VMEM((tokens, m), F32),
            pltpu.VMEM((tokens, ma), F32),
            pltpu.VMEM((2, TILE, m), BF16),
            pltpu.VMEM((2, TILE, ma), BF16),
            pltpu.VMEM((2, nn, TILE), BF16),
            pltpu.VMEM((2, nd, TILE), BF16),
            pltpu.VMEM((nn, m), F32),
            pltpu.VMEM((nd, ma), F32),
            pltpu.VMEM((NCOL, 1, 2 * m + ma + 128), F32),
            pltpu.VMEM((NROW, 1, nn + nd), F32),
            pltpu.VMEM((NROW, 1, 128), F32),
            pltpu.VMEM((NROW, 1, 128), F32),
            pltpu.VMEM((NCOL, 1, 128), F32),
            dma((2, 2)), dma((2, NY, NZ, 2)), dma((4, 3)), dma((4, LONG, 3)), dma((2,)), dma((2,)), dma((NCOL // CHUNK, 2)),
            dma((9, NCOL // CHUNK, 2)), dma((9, NCOL // CHUNK, 2)),
            dma((2, 5)), dma((5,)), dma((5,)),
        ],
        compiler_params=pltpu.CompilerParams(has_side_effects=True, vmem_limit_bytes=VMEM_LIMIT),
        name='fused_step',
    )(dyg, dyu, dyd, xn, xa, wn, wa, wg, wu, wd, r_all, c_all, hyper)


def solution(mesh):
    weight_spec = P('row', 'col')
    act_spec = P(None, 'row')
    grad_spec = P(None, 'col')
    in_specs = (weight_spec,) * 3 + (act_spec, act_spec) + (grad_spec,) * 3 + (P('row'), P('col')) * 3 + (P(),)
    out_specs = (weight_spec,) * 3 + (P('row'), P('col')) * 3 + (act_spec, act_spec)

    def body(w_gate, w_up, w_down, x_norm, x_act, dy_gate, dy_up, dy_down, r_gate, c_gate, r_up, c_up, r_down, c_down, hyper_params):
        m, ng = w_gate.shape
        wg, wu, wd = w_gate.T, w_up.T, w_down.T
        wn = jnp.concatenate([wg.astype(BF16), wu.astype(BF16)], axis=0)
        wa = wd.astype(BF16)
        r_all = jnp.concatenate([r_gate, r_up, r_down])[None]
        c_all = jnp.concatenate([c_gate, c_up, c_down])[None]
        out = fused_step(dy_gate.T, dy_up.T, dy_down.T, x_norm, x_act, wn, wa, wg, wu, wd, r_all, c_all, hyper_params)
        wg, wu, wd, rg, cg, ru, cu, rd, cd, dx_norm, dx_act = finish(*out)
        return (wg.T, wu.T, wd.T, rg[0], cg[0], ru[0], cu[0], rd[0], cd[0], dx_norm, dx_act)

    return jax.shard_map(body, mesh=mesh, in_specs=in_specs, out_specs=out_specs, check_vma=False)
```

```python
import jax
import jax.numpy as jnp
from jax import lax
from jax.experimental import pallas as pl
from jax.experimental.pallas import tpu as pltpu
from jax.sharding import PartitionSpec as P

EPS_ONE = 1e-30
EPS_TWO = 1e-3
MESH = pl.DeviceIdType.MESH
NY, NZ, NX = 4, 8, 4
NCOL, NROW = NY * NZ, NX * 2
LONG = NCOL // 2
BF16, F32 = jnp.bfloat16, jnp.float32


def ring_place(cycle, col):
    y, z = col % NY, col // NY
    u = (y + z) % NY
    if cycle == 0:
        return NY * z + u
    return NY * ((3 * (z - u + NZ)) % NZ) + u


def ring_col(cycle, place):
    place = (place + NCOL) % NCOL
    q, u = place // NY, place % NY
    z = q if cycle == 0 else (3 * q + u) % NZ
    return z * NY + (u - z + NZ) % NY


class Rings:
    def __init__(self, col, row, parts, send_sems, recv_sems):
        self.row, self.parts, self.send_sems, self.recv_sems = row, parts, send_sems, recv_sems
        sign = 1 - 2 * (row % 2)
        self.lanes = []
        for cycle in range(2):
            place = ring_place(cycle, col)
            for way in range(2):
                step_dir = sign if way == 0 else -sign
                self.lanes.append((cycle, way, place, step_dir, ring_col(cycle, place + step_dir)))

    def copy(self, lane, step, k):
        cycle, way, place, step_dir, peer = self.lanes[lane]
        ref = self.parts[k](cycle, ring_col(cycle, place - step_dir * step))
        return pltpu.make_async_remote_copy(
            src_ref=ref, dst_ref=ref, send_sem=self.send_sems.at[lane, k], recv_sem=self.recv_sems.at[lane, step, k],
            device_id=(peer, self.row), device_id_type=MESH)

    def start(self, step):
        for k in range(len(self.parts)):
            for lane in range(4):
                self.guard(lane, step, lambda lane=lane, k=k: self.copy(lane, step, k).start())

    def guard(self, lane, step, go):
        n_steps = LONG - self.lanes[lane][1]
        if isinstance(step, int):
            if step < n_steps:
                go()
        else:
            pl.when(step < n_steps)(go)

    def wait_recv(self, step):
        for k in range(len(self.parts)):
            for lane in range(4):
                self.guard(lane, step, lambda lane=lane, k=k: self.copy(lane, step, k).wait_recv())

    def forward(self, step):
        for k in range(len(self.parts)):
            for lane in range(4):
                self.guard(lane, step - 1, lambda lane=lane, k=k: self.copy(lane, step - 1, k).wait_recv())
                self.guard(lane, step, lambda lane=lane, k=k: self.copy(lane, step, k).start())

    def wait_sends(self, totals):
        for lane in range(4):
            for k, total in enumerate(totals):
                ref = total(LONG - self.lanes[lane][1])
                pltpu.make_async_copy(ref, ref, self.send_sems.at[lane, k]).wait()


class Trees:
    def __init__(self, col, row, pieces, send_sems, recv_sems):
        self.row, self.pieces, self.send_sems, self.recv_sems = row, pieces, send_sems, recv_sems
        self.y, self.z, self.sign = col % NY, col // NY, 1 - 2 * (row % 2)

    def at(self, dy, dz):
        y = (self.y + self.sign * dy + NY) % NY
        z = (self.z + self.sign * dz + NZ) % NZ
        return z * NY + y

    def copy(self, tree, k, origin, target):
        (ey, ez), (fy, fz) = origin, target
        ref = self.pieces[tree][k](self.at(ey, ez))
        return pltpu.make_async_remote_copy(
            src_ref=ref, dst_ref=ref, send_sem=self.send_sems.at[tree, k],
            recv_sem=self.recv_sems.at[tree, (ey - fy) % NY, (ez - fz) % NZ, k],
            device_id=(self.at(fy, fz), self.row), device_id_type=MESH)

    @staticmethod
    def children(tree, ey, ez):
        along_y = {0: [(1, (0, 1)), (-1, (0, 1))], -1: [(1, (0,))], 1: [(-1, (1,))], 2: []}[ey]
        if ez == 0:
            along_z = [1, -1]
        elif ez < 0:
            along_z = [1] if ez > -NZ // 2 else []
        else:
            along_z = [-1] if ez < NZ // 2 - 1 else []
        if tree == 0:
            ys, zs = (along_y if ez == 0 else []), along_z
        else:
            ys, zs = along_y, (along_z if ey == 0 else [])
        return [((0, f), (0, 1)) for f in zs] + [((f, 0), ks) for f, ks in ys]

    def wait(self, tree, k, ey, ez):
        ref = self.pieces[tree][k](self.at(ey, ez))
        pltpu.make_async_copy(ref, ref, self.recv_sems.at[tree, ey % NY, ez % NZ, k]).wait()

    def round(self, r):
        for tree in (1, 0):
            for ez in (0, -1, 1, -2, 2, -3, 3, -4):
                for ey in (0, -1, 1, 2):
                    if abs(ey) + abs(ez) != r:
                        continue
                    if r:
                        for k in range(2):
                            self.wait(tree, k, ey, ez)
                    for target, ks in self.children(tree, ey, ez):
                        for k in ks:
                            self.copy(tree, k, (ey, ez), target).start()


def step_kernel(dyg_ref, dyu_ref, dyd_ref, xn_ref, xa_ref, wg_ref, wu_ref, wd_ref,
                rg_ref, cg_ref, ru_ref, cu_ref, rd_ref, cd_ref, hyper_ref,
                wg_out, wu_out, wd_out, r_out, c_out, dxn_ref, dxa_ref,
                dn_all, dd_all, wn_all, wa_all, acc_n, acc_a,
                xn_buf, xa_buf, dyn_buf, dyd_buf, grad_n, grad_d,
                col_msg, row_msg, u_msg, r_msg, z_msg,
                w_send, w_recv, ag_send, ag_recv, a2a_sent, a2a_recv, x_send, x_recv, tile_sems, st_send, st_recv):
    col, row = lax.axis_index('col'), lax.axis_index('row')
    x, core = row // 2, row % 2
    tokens = dxn_ref.shape[0] // NCOL
    quarter = tokens // NX
    ng = dyg_ref.shape[0]
    nd = dyd_ref.shape[0]
    nn = 2 * ng
    hd = nd // 2
    wn_all[col, pl.ds(0, ng), :] = wg_ref[...].astype(BF16)
    wn_all[col, pl.ds(ng, ng), :] = wu_ref[...].astype(BF16)
    wa_all[col] = wd_ref[...].astype(BF16)

    def w_piece(ref, first, count):
        return lambda origin: ref.at[origin, pl.ds(first, count)]

    w_cuts = (((wn_all, 0, W_CUT), (wa_all, 0, hd)), ((wn_all, W_CUT, nn - W_CUT), (wa_all, hd, hd)))
    trees = Trees(col, row, [[w_piece(*cut) for cut in cuts] for cuts in w_cuts], w_send, w_recv)

    rows_n, rows_d = pl.ds(core * ng, ng), pl.ds(core * hd, hd)

    def shift_of(t):
        return ((2 * (t % 2) - 1) * ((t + 1) // 2) + NCOL) % NCOL

    def a2a_pieces(src, t, peer):
        cols = pl.ds(pl.multiple_of(peer * tokens + x * quarter, quarter), quarter)
        return (src.at[:, cols], dn_all.at[x, t, rows_n]), (dyd_ref.at[rows_d, cols], dd_all.at[x, t, rows_d])

    def a2a_own(src):
        for k, (s, d) in enumerate(a2a_pieces(src, 0, col)):
            pltpu.make_async_copy(s, d, a2a_recv.at[0, k]).start()

    def a2a_send(src, first, last):
        @pl.loop(first, last)
        def _(t):
            peer = (col + shift_of(t)) % NCOL
            for k, (s, d) in enumerate(a2a_pieces(src, t, peer)):
                pltpu.make_async_remote_copy(src_ref=s, dst_ref=d, send_sem=a2a_sent.at[k], recv_sem=a2a_recv.at[t // CHUNK, k],
                                             device_id=(peer, row), device_id_type=MESH).start()

    def by_core(go, *args):
        pl.when(core == 0)(lambda: go(dyg_ref, *args))
        pl.when(core == 1)(lambda: go(dyu_ref, *args))

    def x_of(dx):
        return (x + dx + NX) % NX

    own, prev, succ, far = x, x_of(-1), x_of(1), x_of(2)
    partner = x * 2 + 1 - core
    to_succ, to_prev = succ * 2 + core, prev * 2 + core
    routes = ((own, to_succ, 0, 2), (own, to_prev, 0, 2), (own, partner, 0, 2), (prev, to_succ, 0, 1), (prev, partner, 0, 2),
              (succ, to_prev, 1, 1), (succ, partner, 0, 2), (far, partner, 0, 1), (far, partner, 1, 1))

    def hop(k, ch):
        slot, target, first, count = routes[k]
        cols = pl.ds(ch * CHUNK + first * (CHUNK // 2), count * (CHUNK // 2))
        refs = (dn_all.at[slot, cols, rows_n], dd_all.at[slot, cols, rows_d])
        return [pltpu.make_async_remote_copy(
            src_ref=ref, dst_ref=ref, send_sem=x_send.at[k, ch, p], recv_sem=x_recv.at[k, ch, p],
            device_id=(col, target), device_id_type=MESH) for p, ref in enumerate(refs)]

    def hop_start(ch, *ks):
        for k in ks:
            for copy in hop(k, ch):
                copy.start()

    def hop_wait(ch, *ks):
        for k in ks:
            for copy in hop(k, ch):
                copy.wait_recv()

    def x_first(ch):
        cols = pl.ds(ch * CHUNK, CHUNK)
        for k, ref in enumerate((dn_all.at[x, cols, rows_n], dd_all.at[x, cols, rows_d])):
            pltpu.make_async_copy(ref, ref, a2a_recv.at[ch, k]).wait()
        if DO_X:
            hop_start(ch, 0, 1, 2)

    def x_second(ch):
        if DO_X:
            hop_wait(ch, 0)
            hop_start(ch, 3, 4)
            hop_wait(ch, 1)
            hop_start(ch, 5, 6)

    def x_third(ch):
        if DO_X:
            hop_wait(ch, 3)
            hop_start(ch, 7)
            hop_wait(ch, 5)
            hop_start(ch, 8)

    def x_last(ch):
        if DO_X:
            hop_wait(ch, 2, 4, 6, 7, 8)

    n_chunks = NCOL // CHUNK
    events = {}
    for ch in range(n_chunks):
        for stage, at in zip((x_first, x_second, x_third), X_AT[ch]):
            events.setdefault(at, []).append((stage, ch))

    if DO_A2A:
        by_core(a2a_own)
    grad_n[...] = jnp.zeros_like(grad_n)
    grad_d[...] = jnp.zeros_like(grad_d)
    for r in range(ROUNDS + 1):
        if DO_W:
            trees.round(r)
        if DO_A2A:
            first, last = max(1, A2A_AT[r]), A2A_AT[r + 1]
            if first < last:
                by_core(a2a_send, first, last)
            for stage, ch in events.get(r, ()):
                stage(ch)

    group = 4
    for ch in range(n_chunks):
        if DO_A2A:
            for stage, late in events.get(ROUNDS + 1 + ch, ()):
                stage(late)
            x_last(ch)
        if DO_MM:
            @pl.loop(ch * (CHUNK // group), (ch + 1) * (CHUNK // group))
            def _(g):
                slots = pl.ds(g * group, group)
                js = [(col - shift_of(g * group + i) + NCOL) % NCOL for i in range(group)]
                lhs_n = jnp.concatenate([dn_all[q, slots].reshape(group * nn, quarter) for q in range(NX)], axis=1)
                lhs_d = jnp.concatenate([dd_all[q, slots].reshape(group * nd, quarter) for q in range(NX)], axis=1)
                dims = (((0,), (0,)), ((), ()))
                part_n = lax.dot_general(lhs_n, jnp.concatenate([wn_all[j] for j in js], axis=0), dims, preferred_element_type=F32)
                part_a = lax.dot_general(lhs_d, jnp.concatenate([wa_all[j] for j in js], axis=0), dims, preferred_element_type=F32)

                @pl.when(g == 0)
                def _():
                    acc_n[...] = part_n
                    acc_a[...] = part_a

                @pl.when(g > 0)
                def _():
                    acc_n[...] += part_n
                    acc_a[...] += part_a

    mine = pl.ds(pl.multiple_of(col * tokens, tokens), tokens)
    dxn_ref[mine, :] = acc_n[...].astype(BF16)
    dxa_ref[mine, :] = acc_a[...].astype(BF16)

    def span(ref, offset, count):
        def part(cycle, origin):
            return ref.at[pl.ds(pl.multiple_of(origin * tokens + cycle * (tokens // 2) + offset, 16), count)]
        return part

    sizes = [(dxa_ref, tokens // 4), (dxa_ref, tokens // 4), (dxn_ref, tokens // 2)]
    ag = Rings(col, row, [span(dxa_ref, 0, tokens // 4), span(dxa_ref, tokens // 4, tokens // 4), span(dxn_ref, 0, tokens // 2)],
               ag_send, ag_recv)

    tile = xn_buf.shape[1]
    n_tiles = dxn_ref.shape[0] // tile

    def tile_copies(t, slot):
        at = pl.ds(pl.multiple_of(t * tile, tile), tile)
        pairs = ((xn_ref.at[at], xn_buf.at[slot]), (xa_ref.at[at], xa_buf.at[slot]),
                 (dyg_ref.at[:, at], dyn_buf.at[slot, pl.ds(0, ng)]), (dyu_ref.at[:, at], dyn_buf.at[slot, pl.ds(ng, ng)]),
                 (dyd_ref.at[:, at], dyd_buf.at[slot]))
        return [pltpu.make_async_copy(s, d, tile_sems.at[slot, k]) for k, (s, d) in enumerate(pairs)]

    def dw_tile(t):
        slot = t % 2
        for copy in tile_copies(t, slot):
            copy.wait()

        @pl.when(t + 1 < n_tiles)
        def _():
            for copy in tile_copies(t + 1, 1 - slot):
                copy.start()
        grad_n[...] += jnp.dot(dyn_buf[slot], xn_buf[slot], preferred_element_type=F32)
        grad_d[...] += jnp.dot(dyd_buf[slot], xa_buf[slot], preferred_element_type=F32)

    if DO_DW:
        for copy in tile_copies(0, 0):
            copy.start()
    if DO_AG:
        ag.start(0)
    per_step = n_tiles // DW_STEPS

    @pl.loop(1, DW_STEPS + 1)
    def _(step):
        if DO_AG:
            ag.forward(step)
        if DO_DW:
            @pl.loop(0, per_step)
            def _(k):
                dw_tile((step - 1) * per_step + k)

    def ag_step(step):
        if DO_AG:
            ag.forward(step)

    m = xn_ref.shape[1]
    beta_two, rho, clip = hyper_ref[0], hyper_ref[1], hyper_ref[2]
    n_elem = float(m * NROW * ng * NCOL)
    n_rows, n_cols = float(m * NROW), float(ng * NCOL)
    scales = ((n_rows, n_cols), (n_rows, n_cols), (n_cols, n_rows))

    def lanes_of(values):
        lane = lax.broadcasted_iota(jnp.int32, (1, 128), 1)
        out = jnp.zeros((1, 128), F32)
        for k, value in enumerate(values):
            out = jnp.where(lane == k, value, out)
        return out

    def scatter(k, ref, axis):
        count, mine_at = (NCOL, col) if axis == 'col' else (NROW, row)

        @pl.loop(1, count)
        def _(shift):
            peer = (mine_at + shift) % count
            target = (peer, row) if axis == 'col' else (col, peer)
            pltpu.make_async_remote_copy(src_ref=ref.at[mine_at], dst_ref=ref.at[mine_at], send_sem=st_send.at[k],
                                         recv_sem=st_recv.at[k], device_id=target, device_id_type=MESH).start()

    def collect(k, ref, count):
        part = ref.at[pl.ds(0, count - 1)]
        pltpu.make_async_copy(part, part, st_recv.at[k]).wait()

    def drain(k, ref, count):
        part = ref.at[pl.ds(0, count - 1)]
        pltpu.make_async_copy(part, part, st_send.at[k]).wait()

    def pick(vec, k):
        lane = lax.broadcasted_iota(jnp.int32, (1, 128), 1)
        return jnp.sum(jnp.where(lane == k, vec, 0.0))

    def grads():
        return grad_n[pl.ds(0, ng), :], grad_n[pl.ds(ng, ng), :], grad_d[...]

    ag_step(DW_STEPS + 1)
    squares = [g * g + EPS_ONE for g in grads()]
    w_parts = [jnp.sum(w[...] * w[...]) for w in (wg_ref, wu_ref, wd_ref)]
    row_sums = [jnp.sum(s, axis=0, keepdims=True) for s in squares]
    col_sums = jnp.concatenate([jnp.sum(s, axis=1, keepdims=True) for s in squares], axis=0)
    col_msg[col] = jnp.concatenate(row_sums + [lanes_of(w_parts)], axis=1)
    row_msg[row] = jnp.transpose(jnp.broadcast_to(col_sums, (nn + nd, 128)))[0:1, :]
    if DO_ST:
        scatter(0, col_msg, 'col')
        scatter(1, row_msg, 'row')

    ag_step(DW_STEPS + 2)
    if DO_ST:
        collect(0, col_msg, NCOL)
        collect(1, row_msg, NROW)
    r_total = jnp.sum(col_msg[...], axis=0)
    c_total = jnp.sum(row_msg[...], axis=0)
    n_r = r_total.shape[1] - 128
    lane_r = lax.broadcasted_iota(jnp.int32, (1, n_r), 1)
    lane_c = lax.broadcasted_iota(jnp.int32, (1, nn + nd), 1)
    r_old = jnp.concatenate([rg_ref[...], ru_ref[...], rd_ref[...]], axis=1)
    c_old = jnp.concatenate([cg_ref[...], cu_ref[...], cd_ref[...]], axis=1)
    r_new = beta_two * r_old + (1.0 - beta_two) * (r_total[:, :n_r] / jnp.where(lane_r < 2 * m, n_cols, n_rows))
    c_new = beta_two * c_old + (1.0 - beta_two) * (c_total / jnp.where(lane_c < nn, n_rows, n_cols))
    r_out[...] = r_new
    c_out[...] = c_new
    r_cuts = ((0, m), (m, 2 * m), (2 * m, n_r))
    r_sums = [jnp.sum(r_new[:, a:b]) for a, b in r_cuts]
    w_line = [pick(r_total[:, n_r:], k) for k in range(3)]
    r_msg[row] = lanes_of(r_sums + w_line)
    if DO_ST:
        scatter(2, r_msg, 'row')

    ag_step(DW_STEPS + 3)
    if DO_ST:
        collect(2, r_msg, NROW)
    totals = jnp.sum(r_msg[...], axis=0)
    c_col = jnp.transpose(jnp.broadcast_to(c_out[...], (128, nn + nd)))[:, 0:1]
    c_cols = (c_col[:ng], c_col[ng:nn], c_col[nn:])
    u_sums = []
    new_refs = (wg_out, wu_out, wd_out)
    for k, g in enumerate(grads()):
        r_mean = pick(totals, k) / scales[k][0]
        r_row = r_out[:, r_cuts[k][0]:r_cuts[k][1]]
        update = g * lax.rsqrt(r_row * c_cols[k] / r_mean)
        new_refs[k][...] = update
        u_sums.append(jnp.sum(update * update))
    w_sq = [pick(totals, 3 + k) for k in range(3)]
    u_msg[row] = lanes_of(u_sums)
    if DO_ST:
        scatter(3, u_msg, 'row')

    ag_step(DW_STEPS + 4)
    if DO_ST:
        collect(3, u_msg, NROW)
    z_msg[col] = jnp.sum(u_msg[...], axis=0)
    if DO_ST:
        scatter(4, z_msg, 'col')

    ag_step(DW_STEPS + 5)
    if DO_ST:
        collect(4, z_msg, NCOL)
    u_total = jnp.sum(z_msg[...], axis=0)

    def rms(value):
        return jnp.sqrt(jnp.full((1, 1), value / n_elem, F32))

    for k, (w, out) in enumerate(zip((wg_ref, wu_ref, wd_ref), new_refs)):
        shrink = jnp.maximum(1.0, rms(pick(u_total, k)) / clip)
        step_size = rho * jnp.maximum(EPS_TWO, rms(w_sq[k]))
        out[...] = w[...] - step_size * (out[...] / shrink)

    @pl.loop(DW_STEPS + 6, LONG)
    def _(step):
        ag_step(step)
    if DO_AG:
        ag.wait_recv(LONG - 1)

    if DO_X:
        for ch in range(n_chunks):
            for k in range(len(routes)):
                for copy in hop(k, ch):
                    copy.wait_send()
    if DO_A2A:
        for k, ref in enumerate((dn_all.at[0, pl.ds(0, NCOL - 1), pl.ds(0, ng)], dd_all.at[0, pl.ds(0, NCOL - 1), pl.ds(0, hd)])):
            pltpu.make_async_copy(ref, ref, a2a_sent.at[k]).wait()
    if DO_W:
        for tree, cuts in enumerate(w_cuts):
            for k, (ref, _, count) in enumerate(cuts):
                ref = ref.at[pl.ds(0, NCOL - 1), pl.ds(0, count)]
                pltpu.make_async_copy(ref, ref, w_send.at[tree, k]).wait()
    if DO_AG:
        ag.wait_sends([lambda n, ref=ref, size=size: ref.at[pl.ds(0, n * size)] for ref, size in sizes])
    if DO_ST:
        for k, ref, count in ((0, col_msg, NCOL), (1, row_msg, NROW), (2, r_msg, NROW), (3, u_msg, NROW), (4, z_msg, NCOL)):
            drain(k, ref, count)


DO_W = DO_A2A = DO_X = DO_MM = DO_AG = DO_DW = DO_ST = True
CHUNK, DW_STEPS = 8, 8
ROUNDS = NY // 2 + NZ // 2
A2A_AT = (0, 16, 32, 32, 32, 32, 32, 32)
X_AT = ((1, 2, 3), (1, 2, 3), (2, 3, 4), (2, 4, 5))
W_CUT = 128
TILE = 512


VMEM_LIMIT = 33 * 1024 * 1024
PIECES = 8


def finish_kernel(wg_ref, wu_ref, wd_ref, r_ref, c_ref, dxn_ref, dxa_ref,
                  wg_out, wu_out, wd_out, rg_out, cg_out, ru_out, cu_out, rd_out, cd_out, dxn_out, dxa_out, sems):
    rows = dxn_ref.shape[0] // PIECES
    copies = [pltpu.make_async_copy(src.at[pl.ds(k * rows, rows)], dst.at[pl.ds(k * rows, rows)], sems.at[p, k])
              for p, (src, dst) in enumerate(((dxa_ref, dxa_out), (dxn_ref, dxn_out))) for k in range(PIECES)]
    for copy in copies:
        copy.start()
    for src, dst in ((wg_ref, wg_out), (wu_ref, wu_out), (wd_ref, wd_out)):
        dst[...] = src[...]
    for src, outs in ((r_ref, (rg_out, ru_out, rd_out)), (c_ref, (cg_out, cu_out, cd_out))):
        at = 0
        for out in outs:
            out[...] = src[:, at:at + out.shape[1]]
            at += out.shape[1]
    for copy in copies:
        copy.wait()


def finish(wg, wu, wd, r_all, c_all, dxn, dxa):
    vmem, hbm = pl.BlockSpec(memory_space=pltpu.VMEM), pl.BlockSpec(memory_space=pl.ANY)
    shape = jax.ShapeDtypeStruct
    ng, m = wg.shape
    nd, ma = wd.shape
    stats = [shape((1, n), F32) for n in (m, ng, m, ng, ma, nd)]
    return pl.pallas_call(
        finish_kernel,
        out_shape=[shape(w.shape, F32) for w in (wg, wu, wd)] + stats + [shape(dxn.shape, BF16), shape(dxa.shape, BF16)],
        in_specs=[vmem] * 7,
        out_specs=[vmem] * 9 + [hbm] * 2,
        scratch_shapes=[pltpu.SemaphoreType.DMA((2, PIECES))],
        compiler_params=pltpu.CompilerParams(vmem_limit_bytes=1 * 1024 * 1024),
        name='finish',
    )(wg, wu, wd, r_all, c_all, dxn, dxa)


def fused_step(dyg, dyu, dyd, xn, xa, wg, wu, wd, stats, hyper):
    tokens = xn.shape[0] // NCOL
    ng, nd, m, ma = dyg.shape[0], dyd.shape[0], xn.shape[1], xa.shape[1]
    nn = 2 * ng
    vmem, hbm = pl.BlockSpec(memory_space=pltpu.VMEM), pl.BlockSpec(memory_space=pl.ANY)
    smem = pl.BlockSpec(memory_space=pltpu.SMEM)
    dma = pltpu.SemaphoreType.DMA
    return pl.pallas_call(
        step_kernel,
        out_shape=(pltpu.VMEM(wg.shape, F32), pltpu.VMEM(wu.shape, F32), pltpu.VMEM(wd.shape, F32),
                   pltpu.VMEM((1, 2 * m + ma), F32), pltpu.VMEM((1, nn + nd), F32),
                   pltpu.VMEM(xn.shape, BF16), pltpu.VMEM(xa.shape, BF16)),
        in_specs=[hbm] * 5 + [vmem] * 9 + [smem],
        out_specs=(vmem,) * 7,
        scratch_shapes=[
            pltpu.VMEM((NX, NCOL, nn, tokens // NX), BF16),
            pltpu.VMEM((NX, NCOL, nd, tokens // NX), BF16),
            pltpu.VMEM((NCOL, nn, m), BF16),
            pltpu.VMEM((NCOL, nd, ma), BF16),
            pltpu.VMEM((tokens, m), F32),
            pltpu.VMEM((tokens, ma), F32),
            pltpu.VMEM((2, TILE, m), BF16),
            pltpu.VMEM((2, TILE, ma), BF16),
            pltpu.VMEM((2, nn, TILE), BF16),
            pltpu.VMEM((2, nd, TILE), BF16),
            pltpu.VMEM((nn, m), F32),
            pltpu.VMEM((nd, ma), F32),
            pltpu.VMEM((NCOL, 1, 2 * m + ma + 128), F32),
            pltpu.VMEM((NROW, 1, nn + nd), F32),
            pltpu.VMEM((NROW, 1, 128), F32),
            pltpu.VMEM((NROW, 1, 128), F32),
            pltpu.VMEM((NCOL, 1, 128), F32),
            dma((2, 2)), dma((2, NY, NZ, 2)), dma((4, 3)), dma((4, LONG, 3)), dma((2,)), dma((NCOL // CHUNK, 2)),
            dma((9, NCOL // CHUNK, 2)), dma((9, NCOL // CHUNK, 2)),
            dma((2, 5)), dma((5,)), dma((5,)),
        ],
        compiler_params=pltpu.CompilerParams(has_side_effects=True, vmem_limit_bytes=VMEM_LIMIT),
        name='fused_step',
    )(dyg, dyu, dyd, xn, xa, wg, wu, wd, *stats, hyper)


def solution(mesh):
    weight_spec = P('row', 'col')
    act_spec = P(None, 'row')
    grad_spec = P(None, 'col')
    in_specs = (weight_spec,) * 3 + (act_spec, act_spec) + (grad_spec,) * 3 + (P('row'), P('col')) * 3 + (P(),)
    out_specs = (weight_spec,) * 3 + (P('row'), P('col')) * 3 + (act_spec, act_spec)

    def body(w_gate, w_up, w_down, x_norm, x_act, dy_gate, dy_up, dy_down, r_gate, c_gate, r_up, c_up, r_down, c_down, hyper_params):
        stats = [v[None] for v in (r_gate, c_gate, r_up, c_up, r_down, c_down)]
        out = fused_step(dy_gate.T, dy_up.T, dy_down.T, x_norm, x_act, w_gate.T, w_up.T, w_down.T, stats, hyper_params)
        wg, wu, wd, rg, cg, ru, cu, rd, cd, dx_norm, dx_act = finish(*out)
        return (wg.T, wu.T, wd.T, rg[0], cg[0], ru[0], cu[0], rd[0], cd[0], dx_norm, dx_act)

    return jax.shard_map(body, mesh=mesh, in_specs=in_specs, out_specs=out_specs, check_vma=False)
```
